128 devices in a mesh: ctx: 8 (over z, y_lo), grp: 4 (over y_hi, core), tp: 4 (over x).
Axes of the slice: x: 4, y: 4 (y_hi: 2, y_lo: 2; y = y_hi * 2 + y_lo), z: 4, core: 2. Of those that a mesh axis runs over, the one named last changes fastest.
Arguments:
- tokens: bfloat16 [16384, 4608], P(('grp', 'ctx')), parts along dimension 0, may hold values from -6 to 6
- token_pos: int32 [16384], P(('grp', 'ctx')), parts along dimension 0, may hold values from 0 to 4095, as said below
- norm_gain: float32 [4608], replicated, may hold values from 0.1 to 1.9
- query_weight: bfloat16 [4608, 4096], P('ctx', 'tp'), may hold values from -0.09375 to 0.09375
- key_weight: bfloat16 [4608, 2048], P('ctx', 'tp'), may hold values from -0.09375 to 0.09375
- value_weight: bfloat16 [4608, 2048], P('ctx', 'tp'), may hold values from -0.09375 to 0.09375
Outputs:
- attended: bfloat16 [16384, 4096], P(('grp', 'ctx'), 'tp'), parts along dimension 0
The draws below stay inside these ranges and needn't reach their ends.
There are 4 independent parts, one for each index of `grp`. The reference program is written for one: setup_inputs(seed, part) draws one part's arguments, and reference() takes and returns one part's arrays. A program takes and returns all parts, laid end to end along the dimension named above; an argument that names none is the same for every part. Nothing has to cross between parts.
Inputs may be any that keep to these rules, and one draw needn't show every extreme that they name: `token_pos`: the 512 rows of each index of ctx form two runs of 256 consecutive ascending positions, each starting at a multiple of 256; every position of the sequence occurs exactly once.
All inputs are finite; a program needn't handle non-finite values.
Results may differ from the reference program's by a relative error of at most 0.0077.
Values may be sent and summed in bfloat16 or wider, within the bound.
No kernel may reach another device: no remote copies, remote signals or barrier semaphores. Data moves between devices by JAX's collectives and lax.ppermute only.
A program may use at most 128 MiB of HBM per device.

```python
import jax
import jax.numpy as jnp
from jax import lax

D = 4608
HEADS = 32
KV_HEADS = 16
HEAD_DIM = 128
TOK_DEV = 512
TOKENS = 4096


def draw_token_pos(key, part):
    half = TOK_DEV // 2
    devices = TOKENS // TOK_DEV
    blocks = 2 * devices
    order = jax.random.permutation(jax.random.fold_in(key, 12), blocks).astype(jnp.int32)
    target = (jnp.asarray(part).astype(jnp.int32) % blocks).astype(jnp.int32)
    where_target = jnp.argmax((order == target).astype(jnp.int32)).astype(jnp.int32)
    leading = order[0]
    order = order.at[where_target].set(leading)
    order = order.at[0].set(target)
    starts = order * half
    positions = starts[:, None] + jnp.arange(half, dtype=jnp.int32)[None, :]
    return positions.reshape(-1).astype(jnp.int32)


def levels(own_key, shape, shards, smallest, largest):
    def one(axis_at, shards_of):
        steps = jax.random.uniform(jax.random.fold_in(jax.random.fold_in(own_key, 6), axis_at), (shards_of,), jnp.float32, smallest / len(shards), largest / len(shards))
        return jnp.repeat(jnp.exp(steps), shape[axis_at] // shards_of).reshape((-1,) + (1,) * (len(shape) - axis_at - 1))

    factor_of = one(*shards[0])
    for cut in shards[1:]:
        factor_of = factor_of * one(*cut)
    return factor_of


def normal_values(key, shape, spread, reach, split=(), held_as=jnp.bfloat16):
    result = spread * jax.random.normal(key, shape, jnp.float32)
    if split:
        result = result * levels(key, shape, split, -0.22, 0.18)
    return jnp.clip(result, -reach, reach).astype(held_as)


def setup_inputs(seed: int = 0, part: int = 0) -> dict:
    seeds = jax.random.split(jax.random.key(seed), 7)
    own_keys = jax.random.split(jax.random.fold_in(seeds[6], part), 7)
    tokens = normal_values(own_keys[0], (TOKENS, D), 1.0, 6.0, ((0, 8),))
    token_pos = draw_token_pos(jax.random.fold_in(jax.random.fold_in(seeds[6], part), 71), part)
    norm_gain = jnp.clip(1.0 + 0.18 * jax.random.normal(seeds[2], (D,), jnp.float32), 0.1, 1.9)
    query_weight = normal_values(seeds[3], (D, HEADS * HEAD_DIM), D ** -0.5, 0.09375, ((0, 8), (1, 4)))
    key_weight = normal_values(seeds[4], (D, KV_HEADS * HEAD_DIM), D ** -0.5, 0.09375, ((0, 8), (1, 4)))
    value_weight = normal_values(seeds[5], (D, KV_HEADS * HEAD_DIM), D ** -0.5, 0.09375, ((0, 8), (1, 4)))
    return {"tokens": tokens, "token_pos": token_pos, "norm_gain": norm_gain, "query_weight": query_weight, "key_weight": key_weight, "value_weight": value_weight}


query_scale = 144.0 ** (-0.5)

def rotate(field, positions):
    half = field.shape[-1] // 2
    freq = 10000.0 ** (-jnp.arange(half, dtype=jnp.float32) * 2.0 / field.shape[-1])
    angle = positions.astype(jnp.float32)[:, None] * freq[None, :]
    cosine = jnp.cos(angle)[:, None, :]
    sine = jnp.sin(angle)[:, None, :]
    first = field[..., :half]
    second = field[..., half:]
    return jnp.concatenate([first * cosine - second * sine, second * cosine + first * sine], -1)

def reference(tokens, token_pos, norm_gain, query_weight, key_weight, value_weight):
    count = tokens.shape[0]
    inputs = tokens.astype(jnp.float32)
    normed = (inputs * lax.rsqrt(lax.optimization_barrier(jnp.mean(inputs * inputs, -1, keepdims=True)) + 1e-06) * norm_gain[None, :]).astype(jnp.bfloat16)
    queries = jnp.dot(normed, query_weight, preferred_element_type=jnp.float32).reshape(count, HEADS, HEAD_DIM)
    queries = (rotate(queries, token_pos) * query_scale).astype(jnp.bfloat16)
    keys = jnp.dot(normed, key_weight, preferred_element_type=jnp.float32).reshape(count, KV_HEADS, HEAD_DIM)
    keys = rotate(keys, token_pos).astype(jnp.bfloat16)
    values = jnp.dot(normed, value_weight, preferred_element_type=jnp.float32).astype(jnp.bfloat16)
    values = values.reshape(count, KV_HEADS, HEAD_DIM)
    key_full = lax.optimization_barrier(keys).astype(jnp.float32)
    value_full = lax.optimization_barrier(values).astype(jnp.float32)
    half = TOK_DEV // 2
    query_blocks = queries.reshape(count // half, half, KV_HEADS, 2, HEAD_DIM)
    pos_blocks = token_pos.reshape(count // half, half)

    def block(args):
        query_part, pos_part = args
        query_part = lax.optimization_barrier(query_part).astype(jnp.float32)
        scores = jnp.einsum('ngrd,mgd->grnm', query_part, key_full)
        capped = 50.0 * jnp.tanh(scores / 50.0)
        allowed = token_pos[None, None, None, :] <= pos_part[None, None, :, None]
        weights = jnp.where(allowed, jnp.exp(capped), 0.0).astype(jnp.bfloat16)
        weights = lax.optimization_barrier(weights).astype(jnp.float32)
        numerator = jnp.einsum('grnm,mgd->ngrd', weights, value_full)
        total = lax.optimization_barrier(jnp.sum(weights, -1))
        return (numerator / jnp.transpose(total, (2, 0, 1))[..., None]).astype(jnp.bfloat16)
    attended = lax.map(block, (query_blocks, pos_blocks))
    return attended.reshape(count, HEADS * HEAD_DIM)
```

```python
import functools
import math

import jax
import jax.numpy as jnp
from jax import lax
from jax.experimental import pallas as pl
from jax.experimental.pallas import tpu as pltpu
from jax.sharding import PartitionSpec as P

HEAD_DIM = 128
RUN = 256
ZS = 4
query_scale = 144.0 ** (-0.5)
LINK = ("ctx", "grp")


def route(move):
    pairs = []
    for z in range(ZS):
        for y in range(4):
            for c in range(2):
                z2, y2, c2 = move(z, y, c)
                z2, y2 = z2 % ZS, y2 % 4
                pairs.append(
                    (
                        (z * 2 + y % 2) * 4 + y // 2 * 2 + c,
                        (z2 * 2 + y2 % 2) * 4 + y2 // 2 * 2 + c2,
                    )
                )
    return pairs


Z_UP = route(lambda z, y, c: (z + 1, y, c))
Z_DOWN = route(lambda z, y, c: (z - 1, y, c))
Z_OVER = route(lambda z, y, c: (z + 2, y, c))
Y_IN = route(lambda z, y, c: (z, y ^ 1, c))
Y_OUT = route(lambda z, y, c: (z, y + 1 if y % 2 else y - 1, c))
CORE = route(lambda z, y, c: (z, y, 1 - c))
OUT = [
    route(lambda z, y, c, m=m: ((2 * (z % 2) + c) ^ m, y, z // 2)) for m in range(4)
]


def send(array, pairs):
    return lax.ppermute(array, LINK, pairs)


def norm_kernel(place, tokens_ref, gain_ref, out_ref):
    z, y = place[0], place[1]
    x = tokens_ref[...].astype(jnp.float32)
    scale = lax.rsqrt(jnp.mean(x * x, -1, keepdims=True) + 1e-06)
    width = out_ref.shape[-1]
    for step in range(ZS):
        at = pl.multiple_of(lax.rem(z + step, ZS) * 2 * width, 128)
        part = tokens_ref[:, pl.ds(at, 2 * width)].astype(jnp.float32)
        part = (part * scale * gain_ref[:, pl.ds(at, 2 * width)]).astype(jnp.bfloat16)
        out_ref[2 * step + y] = part[:, :width]
        out_ref[2 * step + 1 - y] = part[:, width:]


def normalise(place, tokens, gain):
    rows, depth = tokens.shape
    block = 128
    width = depth // 8
    return pl.pallas_call(
        norm_kernel,
        grid_spec=pltpu.PrefetchScalarGridSpec(
            num_scalar_prefetch=1,
            grid=(rows // block,),
            in_specs=[
                pl.BlockSpec((block, depth), lambda i, p: (i, 0)),
                pl.BlockSpec((1, depth), lambda i, p: (0, 0)),
            ],
            out_specs=pl.BlockSpec((8, block, width), lambda i, p: (0, i, 0)),
        ),
        out_shape=jax.ShapeDtypeStruct((8, rows, width), jnp.bfloat16),
        cost_estimate=pl.CostEstimate(
            flops=10 * rows * depth, bytes_accessed=4 * rows * depth, transcendentals=rows
        ),
        name="normalise",
    )(place, tokens, gain)


def swap_halves(u):
    return pltpu.roll(u, HEAD_DIM // 2, 1)


def query_kernel(place, sum_ref, cos_ref, sin_ref, out_ref):
    for head in range(2):
        u = sum_ref[:, head * HEAD_DIM : (head + 1) * HEAD_DIM]
        turned = (u * cos_ref[...] + swap_halves(u) * sin_ref[...]) * query_scale
        out_ref[0, :, head * HEAD_DIM : (head + 1) * HEAD_DIM] = turned.astype(jnp.bfloat16)


def key_value_kernel(place, key_ref, value_ref, cos_ref, sin_ref, out_ref):
    u = key_ref[...]
    out_ref[0, :, :HEAD_DIM] = (u * cos_ref[...] + swap_halves(u) * sin_ref[...]).astype(
        jnp.bfloat16
    )
    out_ref[0, :, HEAD_DIM:] = value_ref[...].astype(jnp.bfloat16)


def unit(i, p):
    return lax.rem(p[0] + i, ZS)


def turn_queries(place, sums, cosine, sine):
    rows = sums.shape[0] // 2
    return pl.pallas_call(
        query_kernel,
        grid_spec=pltpu.PrefetchScalarGridSpec(
            num_scalar_prefetch=1,
            grid=(ZS,),
            in_specs=[
                pl.BlockSpec(
                    (rows, 2 * HEAD_DIM), lambda i, p: (unit(i, p) // 2, unit(i, p) % 2)
                ),
                pl.BlockSpec((rows, HEAD_DIM), lambda i, p: (unit(i, p) // 2, 0)),
                pl.BlockSpec((rows, HEAD_DIM), lambda i, p: (unit(i, p) // 2, 0)),
            ],
            out_specs=pl.BlockSpec((1, rows, 2 * HEAD_DIM), lambda i, p: (i, 0, 0)),
        ),
        out_shape=jax.ShapeDtypeStruct((ZS, rows, 2 * HEAD_DIM), jnp.bfloat16),
        name="turn_queries",
    )(place, sums, cosine, sine)


def turn_keys(place, sums, cosine, sine):
    rows = sums.shape[0] // 2
    return pl.pallas_call(
        key_value_kernel,
        grid_spec=pltpu.PrefetchScalarGridSpec(
            num_scalar_prefetch=1,
            grid=(ZS,),
            in_specs=[
                pl.BlockSpec((rows, HEAD_DIM), lambda i, p: (unit(i, p) // 2, unit(i, p) % 2)),
                pl.BlockSpec((rows, HEAD_DIM), lambda i, p: (unit(i, p) // 2, 2 + unit(i, p) % 2)),
                pl.BlockSpec((rows, HEAD_DIM), lambda i, p: (unit(i, p) // 2, 0)),
                pl.BlockSpec((rows, HEAD_DIM), lambda i, p: (unit(i, p) // 2, 0)),
            ],
            out_specs=pl.BlockSpec((1, rows, 2 * HEAD_DIM), lambda i, p: (i, 0, 0)),
        ),
        out_shape=jax.ShapeDtypeStruct((ZS, rows, 2 * HEAD_DIM), jnp.bfloat16),
        name="turn_keys",
    )(place, sums, sums, cosine, sine)


def attend_kernel(place, starts, *refs):
    query_refs, pair_refs = refs[:ZS], refs[ZS : 3 * ZS]
    out_ref = refs[3 * ZS]
    queries, keys, values, acc, order = refs[3 * ZS + 1 :]
    z, c = place[0], place[2]
    for slot in range(16):
        pair = pair_refs[slot // 2][(slot % 2) * RUN : (slot % 2 + 1) * RUN, :]
        keys[slot] = pair[:, :HEAD_DIM].T
        values[slot, :, :HEAD_DIM] = pair[:, HEAD_DIM:]
        values[slot, :, HEAD_DIM:] = jnp.ones((RUN, HEAD_DIM), jnp.bfloat16)
        order[starts[slot]] = slot
    for block in range(2 * ZS):
        for head in range(2):
            queries[block, head * RUN : (head + 1) * RUN, :] = query_refs[block // 2][
                (block % 2) * RUN : (block % 2 + 1) * RUN,
                head * HEAD_DIM : (head + 1) * HEAD_DIM,
            ]

    def weigh(q, slot):
        scores = jnp.dot(q, keys[slot], preferred_element_type=jnp.float32)
        return jnp.exp2(jnp.tanh(scores * (1.0 / 50.0)) * (50.0 * math.log2(math.e)))

    def one_block(block, carry):
        q = queries[block]
        last = starts[4 * (block // 2) + lax.rem(block, 2)]
        row = lax.broadcasted_iota(jnp.int32, (2 * RUN, RUN), 0)
        col = lax.broadcasted_iota(jnp.int32, (2 * RUN, RUN), 1)
        slot = order[last]
        w = jnp.where(col <= (row & (RUN - 1)), weigh(q, slot), 0.0).astype(jnp.bfloat16)
        acc[...] = jnp.dot(w, values[slot], preferred_element_type=jnp.float32)

        def two(i, carry):
            total = acc[...]
            for half in range(2):
                slot = order[2 * i + half]
                w = weigh(q, slot).astype(jnp.bfloat16)
                total = total + jnp.dot(w, values[slot], preferred_element_type=jnp.float32)
            acc[...] = total
            return carry

        lax.fori_loop(0, last // 2, two, 0)

        @pl.when(lax.rem(last, 2) == 1)
        def _():
            slot = order[last - 1]
            w = weigh(q, slot).astype(jnp.bfloat16)
            acc[...] += jnp.dot(w, values[slot], preferred_element_type=jnp.float32)

        result = (acc[:, :HEAD_DIM] / acc[:, HEAD_DIM:]).astype(jnp.bfloat16)
        target = lax.rem(z + block // 2, ZS) ^ (2 * lax.rem(z, 2) + c)
        at = pl.multiple_of(lax.rem(block, 2) * RUN, RUN)
        out_ref[target, pl.ds(at, RUN), :HEAD_DIM] = result[:RUN]
        out_ref[target, pl.ds(at, RUN), HEAD_DIM:] = result[RUN:]
        return carry

    lax.fori_loop(0, 2 * ZS, one_block, 0)


def attend(place, starts, query_parts, pair_parts):
    rows = query_parts[0].shape[0]
    whole = pl.BlockSpec(memory_space=pltpu.VMEM)
    scalar = pl.BlockSpec(memory_space=pltpu.SMEM)
    return pl.pallas_call(
        attend_kernel,
        in_specs=[scalar, scalar] + [whole] * (3 * ZS),
        out_specs=whole,
        out_shape=jax.ShapeDtypeStruct((ZS, rows, 2 * HEAD_DIM), jnp.bfloat16),
        scratch_shapes=[
            pltpu.VMEM((2 * ZS, 2 * RUN, HEAD_DIM), jnp.bfloat16),
            pltpu.VMEM((16, HEAD_DIM, RUN), jnp.bfloat16),
            pltpu.VMEM((16, RUN, 2 * HEAD_DIM), jnp.bfloat16),
            pltpu.VMEM((2 * RUN, 2 * HEAD_DIM), jnp.float32),
            pltpu.SMEM((16,), jnp.int32),
        ],
        name="attend",
    )(place, starts, *query_parts, *pair_parts)


def exchange_z(parts):
    return [
        parts[0],
        send(parts[3], Z_DOWN),
        send(parts[2], Z_OVER),
        send(parts[1], Z_UP),
    ]


def on_device(tokens, token_pos, norm_gain, query_weight, key_weight, value_weight):
    rows, depth = tokens.shape
    ctx, grp = lax.axis_index("ctx"), lax.axis_index("grp")
    z, y, c = ctx // 2, ctx % 2, grp % 2
    place = jnp.stack([z, y, c]).astype(jnp.int32)

    half = HEAD_DIM * 2
    pick = lambda w, n: lax.dynamic_slice_in_dim(w, c * n, n, 1)
    pair_own = jnp.concatenate([pick(key_weight, half), pick(value_weight, half)], 1)
    query_own = pick(query_weight, 2 * half)

    pair = [None] * 8
    query = [None] * 8
    pair[0], query[0] = pair_own, query_own
    pair[2], pair[6] = send(pair[0], Z_DOWN), send(pair[0], Z_UP)
    pair[1], query[1] = send(pair[0], Y_OUT), send(query[0], Y_IN)
    query[2], query[6] = send(query[0], Z_DOWN), send(query[0], Z_UP)
    pair[3], pair[7] = send(pair[2], Y_IN), send(pair[6], Y_OUT)
    pair[4], query[4] = send(pair[2], Z_DOWN), send(query[6], Z_UP)
    query[3], query[7] = send(query[2], Y_IN), send(query[6], Y_OUT)
    pair[5], query[5] = send(pair[4], Y_OUT), send(query[4], Y_IN)

    other_tokens = send(tokens, CORE)
    other_pos = send(token_pos, CORE)
    pos = jnp.where(c == 0, jnp.stack([token_pos, other_pos]), jnp.stack([other_pos, token_pos]))
    gain = norm_gain[None, :]
    own, other = normalise(place, tokens, gain), normalise(place, other_tokens, gain)

    firsts = pos.reshape(2, 2, RUN)[:, :, 0] // RUN
    firsts = jnp.stack([firsts, send(firsts, Y_IN)])
    firsts = jnp.stack(
        [firsts, send(firsts, Z_DOWN), send(firsts, Z_OVER), send(firsts, Z_UP)]
    )
    starts = jnp.where(z // 2 == 0, firsts[:, :, 0], firsts[:, :, 1]).reshape(16)

    freq = 10000.0 ** (-jnp.arange(HEAD_DIM // 2, dtype=jnp.float32) * 2.0 / HEAD_DIM)
    angle = pos.reshape(2 * rows).astype(jnp.float32)[:, None] * freq[None, :]
    cosine, sine = jnp.cos(angle), jnp.sin(angle)
    cosine = jnp.concatenate([cosine, cosine], 1)
    sine = jnp.concatenate([-sine, sine], 1)

    def project(pieces):
        def one(normed):
            total = None
            for i in (0, 1, 2, 6, 3, 7, 4, 5):
                part = jnp.dot(normed[i], pieces[i], preferred_element_type=jnp.float32)
                total = part if total is None else total + part
            return total

        mine, theirs = one(own), one(other)
        return jnp.where(
            c == 0, jnp.concatenate([mine, theirs]), jnp.concatenate([theirs, mine])
        )

    pair_units = turn_keys(place, project(pair), cosine, sine)
    pair_parts = exchange_z([pair_units[d] for d in range(ZS)])
    across = [send(p, Y_IN) for p in pair_parts]
    pair_parts = [p for both in zip(pair_parts, across) for p in both]

    query_units = turn_queries(place, project(query), cosine, sine)
    query_parts = exchange_z([query_units[d] for d in range(ZS)])

    parts = attend(place, starts, query_parts, pair_parts)
    result = jnp.zeros((rows, 8 * HEAD_DIM), jnp.bfloat16)
    for m in range(ZS):
        source = z ^ m
        at = (source % 2) * 4 * HEAD_DIM + (source // 2) * 2 * HEAD_DIM
        result = lax.dynamic_update_slice_in_dim(result, send(parts[m], OUT[m]), at, 1)
    return result


def solution(mesh):
    in_specs = (
        P(("grp", "ctx"), None),
        P(("grp", "ctx")),
        P(),
        P("ctx", "tp"),
        P("ctx", "tp"),
        P("ctx", "tp"),
    )
    out_specs = P(("grp", "ctx"), "tp")
    return jax.shard_map(
        on_device, mesh=mesh, in_specs=in_specs, out_specs=out_specs, check_vma=False
    )
```

```python
import functools
import math

import jax
import jax.numpy as jnp
from jax import lax
from jax.experimental import pallas as pl
from jax.experimental.pallas import tpu as pltpu
from jax.sharding import PartitionSpec as P

HEAD_DIM = 128
RUN = 256
ZS = 4
query_scale = 144.0 ** (-0.5)
LINK = ("ctx", "grp")


def route(move):
    pairs = []
    for z in range(ZS):
        for y in range(4):
            for c in range(2):
                z2, y2, c2 = move(z, y, c)
                z2, y2 = z2 % ZS, y2 % 4
                pairs.append(
                    (
                        (z * 2 + y % 2) * 4 + y // 2 * 2 + c,
                        (z2 * 2 + y2 % 2) * 4 + y2 // 2 * 2 + c2,
                    )
                )
    return pairs


Z_UP = route(lambda z, y, c: (z + 1, y, c))
Z_DOWN = route(lambda z, y, c: (z - 1, y, c))
Z_OVER = route(lambda z, y, c: (z + 2, y, c))
Y_IN = route(lambda z, y, c: (z, y ^ 1, c))
Y_OUT = route(lambda z, y, c: (z, y + 1 if y % 2 else y - 1, c))
CORE = route(lambda z, y, c: (z, y, 1 - c))
OUT = [
    route(lambda z, y, c, m=m: ((2 * (z % 2) + c) ^ m, y, z // 2)) for m in range(4)
]


def send(array, pairs):
    return lax.ppermute(array, LINK, pairs)


def norm_kernel(tokens_ref, gain_ref, out_ref):
    x = tokens_ref[...].astype(jnp.float32)
    scale = lax.rsqrt(jnp.mean(x * x, -1, keepdims=True) + 1e-06)
    out_ref[...] = (x * scale * gain_ref[...]).astype(jnp.bfloat16)


def normalise(tokens, gain):
    rows, depth = tokens.shape
    block = 64
    return pl.pallas_call(
        norm_kernel,
        grid=(rows // block,),
        in_specs=[
            pl.BlockSpec((block, depth), lambda i: (i, 0)),
            pl.BlockSpec((1, depth), lambda i: (0, 0)),
        ],
        out_specs=pl.BlockSpec((block, depth), lambda i: (i, 0)),
        out_shape=jax.ShapeDtypeStruct((rows, depth), jnp.bfloat16),
        cost_estimate=pl.CostEstimate(
            flops=10 * rows * depth, bytes_accessed=4 * rows * depth, transcendentals=rows
        ),
        name="normalise",
    )(tokens, gain)


def swap_halves(u):
    return pltpu.roll(u, HEAD_DIM // 2, 1)


def project_kernel(offsets, kind, started, place, *refs):
    refs = list(refs)
    take = lambda n: [refs.pop(0) for _ in range(n)]
    inputs = take(2)
    pieces = take(2 * len(offsets))
    begun = take(1)[0] if started else None
    tables = take(2) if kind else None
    marks = take(1)[0] if kind == "pair" else None
    outs = take(ZS if kind else 1)
    both = take(1)[0]
    sums = take(1)[0] if kind else outs[0]
    z, y, c = place[0], place[1], place[2]
    height = pieces[0].shape[0]
    for i in range(len(offsets)):
        for other in range(2):
            at = pl.multiple_of((y if other == 0 else 1 - y) * height, 16)
            both[i, pl.ds(at, height), :] = pieces[2 * i + other][...]
    rows = inputs[0].shape[0]
    for side in range(2):

        def part(j, carry, side=side):
            at = pl.ds(pl.multiple_of(j * RUN, RUN), RUN)
            total = None
            for i, d in enumerate(offsets):
                lanes = pl.multiple_of(lax.rem(z + d, ZS) * 2 * height, 128)
                got = jnp.dot(
                    inputs[side][at, pl.ds(lanes, 2 * height)],
                    both[i],
                    preferred_element_type=jnp.float32,
                )
                total = got if total is None else total + got
            if started:
                total = total + begun[side, at, :]
            sums[side, at, :] = total
            return carry

        lax.fori_loop(0, rows // RUN, part, 0)
    if not kind:
        return
    cosine, sine = tables
    for d in range(ZS):
        u = lax.rem(z + d, ZS)
        side, head = (u // 2) ^ c, lax.rem(u, 2)

        def turned(at):
            lanes = pl.ds(pl.multiple_of(at, HEAD_DIM), HEAD_DIM)
            x = sums[side, :, lanes]
            return x * cosine[side] + swap_halves(x) * sine[side]

        if kind == "pair":
            outs[d][:rows, :HEAD_DIM] = turned(head * HEAD_DIM).astype(jnp.bfloat16)
            lanes = pl.ds(pl.multiple_of((2 + head) * HEAD_DIM, HEAD_DIM), HEAD_DIM)
            outs[d][:rows, HEAD_DIM:] = sums[side, :, lanes].astype(jnp.bfloat16)
            outs[d][rows:, :] = marks[side]
        else:
            for k in range(2):
                outs[d][:, k * HEAD_DIM : (k + 1) * HEAD_DIM] = (
                    turned((2 * head + k) * HEAD_DIM) * query_scale
                ).astype(jnp.bfloat16)


def project(place, inputs, pieces, offsets, kind=None, begun=None, tables=(), marks=None):
    rows, depth = inputs[0].shape
    height, columns = pieces[0].shape
    whole = pl.BlockSpec(memory_space=pltpu.VMEM)
    scalar = pl.BlockSpec(memory_space=pltpu.SMEM)
    chosen = [pieces[2 * d + other] for d in offsets for other in range(2)]
    args = [*inputs, *chosen]
    args += [] if begun is None else [begun]
    args += [*tables] + ([] if marks is None else [marks])
    sums = (2, rows, columns)
    scratch = [pltpu.VMEM((len(offsets), 2 * height, columns), jnp.bfloat16)]
    if kind:
        tall = rows + 16 if kind == "pair" else rows
        out_shape = [jax.ShapeDtypeStruct((tall, 2 * HEAD_DIM), jnp.bfloat16)] * ZS
        scratch.append(pltpu.VMEM(sums, jnp.float32))
    else:
        out_shape = [jax.ShapeDtypeStruct(sums, jnp.float32)]
    out = pl.pallas_call(
        functools.partial(project_kernel, offsets, kind, begun is not None),
        in_specs=[scalar] + [whole] * len(args),
        out_specs=[whole] * len(out_shape),
        out_shape=out_shape,
        scratch_shapes=scratch,
        cost_estimate=pl.CostEstimate(
            flops=8 * rows * height * len(offsets) * columns,
            bytes_accessed=4 * rows * depth,
            transcendentals=0,
        ),
        name="project_" + (kind or "part"),
    )(place, *args)
    return out if kind else out[0]


def attend_kernel(place, starts, *refs):
    query_refs, pair_refs = refs[:ZS], refs[ZS : 3 * ZS]
    out_ref = refs[3 * ZS]
    queries, keys, values, acc, order = refs[3 * ZS + 1 :]
    z, c = place[0], place[2]
    for slot in range(16):
        pair = pair_refs[slot // 2][(slot % 2) * RUN : (slot % 2 + 1) * RUN, :]
        keys[slot] = pair[:, :HEAD_DIM].T
        values[slot, :, :HEAD_DIM] = pair[:, HEAD_DIM:]
        values[slot, :, HEAD_DIM:] = jnp.ones((RUN, HEAD_DIM), jnp.bfloat16)
        order[starts[slot]] = slot
    for block in range(2 * ZS):
        for head in range(2):
            queries[block, head * RUN : (head + 1) * RUN, :] = query_refs[block // 2][
                (block % 2) * RUN : (block % 2 + 1) * RUN,
                head * HEAD_DIM : (head + 1) * HEAD_DIM,
            ]

    def weigh(q, slot):
        scores = jnp.dot(q, keys[slot], preferred_element_type=jnp.float32)
        return jnp.exp2(jnp.tanh(scores * (1.0 / 50.0)) * (50.0 * math.log2(math.e)))

    def one_block(block, carry):
        q = queries[block]
        last = starts[4 * (block // 2) + lax.rem(block, 2)]
        row = lax.broadcasted_iota(jnp.int32, (2 * RUN, RUN), 0)
        col = lax.broadcasted_iota(jnp.int32, (2 * RUN, RUN), 1)
        slot = order[last]
        w = jnp.where(col <= (row & (RUN - 1)), weigh(q, slot), 0.0).astype(jnp.bfloat16)
        acc[...] = jnp.dot(w, values[slot], preferred_element_type=jnp.float32)

        def two(i, carry):
            total = acc[...]
            for half in range(2):
                slot = order[2 * i + half]
                w = weigh(q, slot).astype(jnp.bfloat16)
                total = total + jnp.dot(w, values[slot], preferred_element_type=jnp.float32)
            acc[...] = total
            return carry

        lax.fori_loop(0, last // 2, two, 0)

        @pl.when(lax.rem(last, 2) == 1)
        def _():
            slot = order[last - 1]
            w = weigh(q, slot).astype(jnp.bfloat16)
            acc[...] += jnp.dot(w, values[slot], preferred_element_type=jnp.float32)

        result = (acc[:, :HEAD_DIM] / acc[:, HEAD_DIM:]).astype(jnp.bfloat16)
        target = lax.rem(z + block // 2, ZS) ^ (2 * lax.rem(z, 2) + c)
        at = pl.multiple_of(lax.rem(block, 2) * RUN, RUN)
        out_ref[target, pl.ds(at, RUN), :HEAD_DIM] = result[:RUN]
        out_ref[target, pl.ds(at, RUN), HEAD_DIM:] = result[RUN:]
        return carry

    lax.fori_loop(0, 2 * ZS, one_block, 0)


def attend(place, starts, query_parts, pair_parts):
    rows = query_parts[0].shape[0]
    whole = pl.BlockSpec(memory_space=pltpu.VMEM)
    scalar = pl.BlockSpec(memory_space=pltpu.SMEM)
    return pl.pallas_call(
        attend_kernel,
        in_specs=[scalar, scalar] + [whole] * (3 * ZS),
        out_specs=whole,
        out_shape=jax.ShapeDtypeStruct((ZS, rows, 2 * HEAD_DIM), jnp.bfloat16),
        scratch_shapes=[
            pltpu.VMEM((2 * ZS, 2 * RUN, HEAD_DIM), jnp.bfloat16),
            pltpu.VMEM((16, HEAD_DIM, RUN), jnp.bfloat16),
            pltpu.VMEM((16, RUN, 2 * HEAD_DIM), jnp.bfloat16),
            pltpu.VMEM((2 * RUN, 2 * HEAD_DIM), jnp.float32),
            pltpu.SMEM((16,), jnp.int32),
        ],
        name="attend",
    )(place, starts, *query_parts, *pair_parts)


def exchange_z(parts):
    return [
        parts[0],
        send(parts[3], Z_DOWN),
        send(parts[2], Z_OVER),
        send(parts[1], Z_UP),
    ]


def after(first, *rest):
    return lax.optimization_barrier((*rest, first))[: len(rest)]


def on_device(tokens, token_pos, norm_gain, query_weight, key_weight, value_weight):
    rows, depth = tokens.shape
    ctx, grp = lax.axis_index("ctx"), lax.axis_index("grp")
    z, y, c = ctx // 2, ctx % 2, grp % 2
    place = jnp.stack([z, y, c]).astype(jnp.int32)

    half = HEAD_DIM * 2
    pick = lambda w, n: lax.dynamic_slice_in_dim(w, c * n, n, 1)
    pair_own = jnp.concatenate([pick(key_weight, half), pick(value_weight, half)], 1)
    query_own = pick(query_weight, 2 * half)

    pair = [None] * 8
    query = [None] * 8
    pair[0], query[0] = pair_own, query_own
    pair[2], pair[6] = send(pair[0], Z_DOWN), send(pair[0], Z_UP)
    pair[1], query[1] = send(pair[0], Y_OUT), send(query[0], Y_IN)
    other_tokens, other_pos = send(tokens, CORE), send(token_pos, CORE)
    query[2], query[6] = send(query[0], Z_DOWN), send(query[0], Z_UP)
    gain = norm_gain[None, :]
    own = normalise(tokens, gain)

    pair[2], pair[6], own = lax.optimization_barrier((pair[2], pair[6], own))
    pair[3], pair[7] = send(pair[2], Y_IN), send(pair[6], Y_OUT)
    pair[4], query[4] = send(pair[2], Z_DOWN), send(query[6], Z_UP)
    (other_tokens,) = after(own, other_tokens)
    other = normalise(other_tokens, gain)
    query[3], query[7] = send(query[2], Y_IN), send(query[6], Y_OUT)
    pair[5], query[5] = send(pair[4], Y_OUT), send(query[4], Y_IN)
    inputs = (own, other)

    pos = jnp.stack([token_pos, other_pos])
    freq = 10000.0 ** (-jnp.arange(HEAD_DIM // 2, dtype=jnp.float32) * 2.0 / HEAD_DIM)
    angle = pos.astype(jnp.float32)[:, :, None] * freq[None, None, :]
    cosine, sine = jnp.cos(angle), jnp.sin(angle)
    tables = (jnp.concatenate([cosine, cosine], 2), jnp.concatenate([-sine, sine], 2))
    firsts = (pos.reshape(2, 2, RUN)[:, :, 0] // RUN).astype(jnp.bfloat16)
    marks = jnp.broadcast_to(firsts[:, None, :, None], (2, 16, 2, HEAD_DIM))
    marks = marks.reshape(2, 16, 2 * HEAD_DIM)

    begun = project(place, inputs, pair, (0, 1, 3))
    pair_parts = project(place, inputs, pair, (2,), "pair", begun, tables, marks)
    pair_parts = exchange_z(pair_parts)
    across = [send(p, Y_IN) for p in pair_parts]
    pair_parts = [p for both in zip(pair_parts, across) for p in both]
    starts = jnp.stack([p[rows, at] for p in pair_parts for at in (0, HEAD_DIM)])
    starts = starts.astype(jnp.int32)

    begun = project(place, inputs, query, (0, 1, 3))
    query_parts = project(place, inputs, query, (2,), "query", begun, tables)
    query_parts = exchange_z(query_parts)

    parts = attend(place, starts, query_parts, pair_parts)
    result = jnp.zeros((rows, 8 * HEAD_DIM), jnp.bfloat16)
    for m in range(ZS):
        source = z ^ m
        at = (source % 2) * 4 * HEAD_DIM + (source // 2) * 2 * HEAD_DIM
        result = lax.dynamic_update_slice_in_dim(result, send(parts[m], OUT[m]), at, 1)
    return result


def solution(mesh):
    in_specs = (
        P(("grp", "ctx"), None),
        P(("grp", "ctx")),
        P(),
        P("ctx", "tp"),
        P("ctx", "tp"),
        P("ctx", "tp"),
    )
    out_specs = P(("grp", "ctx"), "tp")
    return jax.shard_map(
        on_device, mesh=mesh, in_specs=in_specs, out_specs=out_specs, check_vma=False
    )
```
